32 devices in a mesh: dp: 8 (over z, y), tensor: 4 (over x, core).
Axes of the slice: x: 2, y: 2, z: 4, core: 2. Of those that a mesh axis runs over, the one named last changes fastest.
Arguments:
- hidden_in: bfloat16 [10240, 2048], P(('dp', 'tensor')), may hold values from -6 to 6
- segment: int32 [10240], P('dp'), may hold values from 0 to 2, as said below
- position: int32 [10240], P('dp'), may hold values from 0 to 5374, as said below
- attn_gain: bfloat16 [2048], P('dp'), may hold values from 0.25 to 1.75
- w_query: bfloat16 [2048, 2048], P('dp', 'tensor'), may hold values from -0.125 to 0.125
- key_weight: bfloat16 [2048, 1024], P('dp', 'tensor'), may hold values from -0.125 to 0.125
- value_weight: bfloat16 [2048, 1024], P('dp', 'tensor'), may hold values from -0.125 to 0.125
- w_headgate: bfloat16 [2048, 16], P('dp', 'tensor'), may hold values from -0.125 to 0.125
- query_gain: bfloat16 [128], P('dp'), may hold values from 0.25 to 1.75
- key_gain: bfloat16 [128], P('dp'), may hold values from 0.25 to 1.75
- w_out: bfloat16 [2048, 2048], P('tensor', 'dp'), may hold values from -3 to 3
- mlp_gain: bfloat16 [2048], P('dp'), may hold values from 0.25 to 1.75
- w_gate: bfloat16 [2048, 6144], P('dp', 'tensor'), may hold values from -0.125 to 0.125
- w_up: bfloat16 [2048, 6144], P('dp', 'tensor'), may hold values from -0.125 to 0.125
- w_down: bfloat16 [6144, 2048], P('tensor', 'dp'), may hold values from -0.078125 to 0.078125
- cotangent: bfloat16 [10240, 2048], P(('dp', 'tensor')), may hold values from -6 to 6
Outputs:
- layer_out: bfloat16 [10240, 2048], P(('dp', 'tensor'))
- grad_in: bfloat16 [10240, 2048], P(('dp', 'tensor'))
- grad_attn_gain: float32 [2048], P('dp')
- grad_query: float32 [2048, 2048], P('dp', 'tensor')
- grad_key: float32 [2048, 1024], P('dp', 'tensor')
- grad_value: float32 [2048, 1024], P('dp', 'tensor')
- grad_headgate: float32 [2048, 16], P('dp', 'tensor')
- grad_query_gain: float32 [128], P('dp')
- grad_key_gain: float32 [128], P('dp')
- grad_out: float32 [2048, 2048], P('tensor', 'dp')
- grad_mlp_gain: float32 [2048], P('dp')
- grad_gate: float32 [2048, 6144], P('dp', 'tensor')
- grad_up: float32 [2048, 6144], P('dp', 'tensor')
- grad_down: float32 [6144, 2048], P('tensor', 'dp')
The draws below stay inside these ranges and needn't reach their ends.
Inputs may be any that keep to these rules, and one draw needn't show every extreme that they name: Within each group the segment ids never fall: a prompt of 768 to 1024 tokens (id 0), then continuation 1, then continuation 2, each of 1 to 256 tokens. Some group has a prompt of exactly 1024 tokens and some group a continuation of exactly 256 tokens. A group's prompt has consecutive positions from a start that differs by group; each continuation's positions follow on from the end of the prompt. Some group starts at 0 and some group reaches the largest position.
All inputs are finite; a program needn't handle non-finite values.
Results may differ from the reference program's by a relative error of at most 0.025.
Values may be sent and summed in bfloat16 or wider, within the bound.
A program may use at most 256 MiB of HBM per device.

```python
import jax
import jax.numpy as jnp
from jax import lax

MODEL_WIDTH = 2048
QUERY_HEADS = 16
KEY_VALUE_HEADS = 8
HEAD_WIDTH = 128
FF = 6144
PROMPT_MAX = 1024
CONT_MAX = 256
POS_SPAN = 4096
GROUP_TOK = 1280
TOKENS = 10240


def group_layout(key):
    groups = TOKENS // GROUP_TOK
    keys = jax.random.split(jax.random.fold_in(key, 7), 5)
    shortest = GROUP_TOK - 2 * CONT_MAX
    prompt_len = jax.random.randint(keys[0], (groups,), shortest, PROMPT_MAX + 1)
    longest_at = jax.random.randint(keys[1], (), 0, groups)
    short_at = (longest_at + 1 + jax.random.randint(keys[2], (), 0, groups - 1)) % groups
    group_ids = jnp.arange(groups)
    prompt_len = jnp.where(group_ids == longest_at, PROMPT_MAX, prompt_len)
    prompt_len = jnp.where(group_ids == short_at, shortest, prompt_len)
    remain = GROUP_TOK - prompt_len
    first_low = jnp.maximum(remain - CONT_MAX, 1)
    first_high = jnp.minimum(remain - 1, CONT_MAX)
    first_len = jax.random.randint(keys[3], (groups,), first_low, first_high + 1)
    index = jnp.arange(GROUP_TOK)[None, :]
    in_first = (index >= prompt_len[:, None]).astype(jnp.int32)
    in_second = (index >= (prompt_len + first_len)[:, None]).astype(jnp.int32)
    segment_ids = in_first + in_second
    start = jax.random.randint(keys[4], (groups,), 0, POS_SPAN)
    offset = jnp.where(segment_ids == 2, index - first_len[:, None], index)
    top_offset = jnp.max(offset, axis=1)
    start = jnp.where(group_ids == longest_at, 0, start)
    start = jnp.where(group_ids == short_at, POS_SPAN - 1 + (GROUP_TOK - 1 - top_offset), start)
    positions = start[:, None] + offset
    return (segment_ids.reshape(-1).astype(jnp.int32), positions.reshape(-1).astype(jnp.int32))


def draw_segment(key, part):
    segment_ids, positions = group_layout(key)
    return segment_ids


def draw_position(key, part):
    segment_ids, positions = group_layout(key)
    return positions


def steps_of(key, dims, cuts, least, largest):
    def one(dim, shards_of):
        steps = jax.random.uniform(jax.random.fold_in(jax.random.fold_in(key, 6), dim), (shards_of,), jnp.float32, least / len(cuts), largest / len(cuts))
        return jnp.repeat(jnp.exp(steps), dims[dim] // shards_of).reshape((-1,) + (1,) * (len(dims) - dim - 1))

    loudness = one(*cuts[0])
    for cut in cuts[1:]:
        loudness = loudness * one(*cut)
    return loudness


def scatter_about(own_key, dims, spread, limit, cuts=(), held_as=jnp.bfloat16):
    drawn = jax.random.normal(own_key, dims, jnp.float32) * spread
    if len(cuts) > 0:
        drawn = steps_of(own_key, dims, cuts, -0.22, 0.18) * drawn
    return jnp.clip(drawn, min=-limit, max=limit).astype(held_as)


def setup_inputs(seed: int = 0) -> dict:
    splits = jax.random.split(jax.random.key(seed), 17)
    return {
        "hidden_in": scatter_about(splits[0], (TOKENS, MODEL_WIDTH), 1.0, 6.0, ((0, 32),)),
        "segment": draw_segment(jax.random.fold_in(splits[16], 71), 0),
        "position": draw_position(jax.random.fold_in(splits[16], 71), 0),
        "attn_gain": jnp.clip(1.0 + 0.15 * jax.random.normal(splits[3], (MODEL_WIDTH,), jnp.float32), 0.25, 1.75).astype(jnp.bfloat16),
        "w_query": scatter_about(splits[4], (MODEL_WIDTH, QUERY_HEADS * HEAD_WIDTH), MODEL_WIDTH ** -0.5, 0.125, ((0, 8), (1, 4))),
        "key_weight": scatter_about(splits[5], (MODEL_WIDTH, KEY_VALUE_HEADS * HEAD_WIDTH), MODEL_WIDTH ** -0.5, 0.125, ((0, 8), (1, 4))),
        "value_weight": scatter_about(splits[6], (MODEL_WIDTH, KEY_VALUE_HEADS * HEAD_WIDTH), MODEL_WIDTH ** -0.5, 0.125, ((0, 8), (1, 4))),
        "w_headgate": scatter_about(splits[7], (MODEL_WIDTH, QUERY_HEADS), MODEL_WIDTH ** -0.5, 0.125, ((0, 8), (1, 4))),
        "query_gain": jnp.clip(1.0 + 0.15 * jax.random.normal(splits[8], (HEAD_WIDTH,), jnp.float32), 0.25, 1.75).astype(jnp.bfloat16),
        "key_gain": jnp.clip(1.0 + 0.15 * jax.random.normal(splits[9], (HEAD_WIDTH,), jnp.float32), 0.25, 1.75).astype(jnp.bfloat16),
        "w_out": scatter_about(splits[10], (QUERY_HEADS * HEAD_WIDTH, MODEL_WIDTH), (max(QUERY_HEADS * HEAD_WIDTH // 512, 1)) ** -0.5, 3.0, ((0, 4), (1, 8))),
        "mlp_gain": jnp.clip(1.0 + 0.15 * jax.random.normal(splits[11], (MODEL_WIDTH,), jnp.float32), 0.25, 1.75).astype(jnp.bfloat16),
        "w_gate": scatter_about(splits[12], (MODEL_WIDTH, FF), MODEL_WIDTH ** -0.5, 0.125, ((0, 8), (1, 4))),
        "w_up": scatter_about(splits[13], (MODEL_WIDTH, FF), MODEL_WIDTH ** -0.5, 0.125, ((0, 8), (1, 4))),
        "w_down": scatter_about(splits[14], (FF, MODEL_WIDTH), FF ** -0.5, 0.078125, ((0, 4), (1, 8))),
        "cotangent": scatter_about(splits[15], (TOKENS, MODEL_WIDTH), 1.0, 6.0, ((0, 32),)),
    }


EPS = 1e-06
THETA = 1000000.0
NEG = -1e+30

@jax.custom_vjp
def lower_precision(v):
    return lax.optimization_barrier(v.astype(jnp.bfloat16)).astype(jnp.float32)

@jax.custom_vjp
def lower_precision_back(v):
    return v

def low_keep(v):
    return (lower_precision(v), None)

def low_pass(kept, grad):
    return (grad,)

def back_keep(v):
    return (v, None)

def back_low(kept, grad):
    return (lower_precision(grad),)
lower_precision.defvjp(low_keep, low_pass)
lower_precision_back.defvjp(back_keep, back_low)

def matrix_product(left, right):
    return jnp.dot(left, right, precision=lax.Precision.HIGHEST)

def root_mean_rows(value_rows, gain):
    return value_rows * lax.rsqrt(lax.optimization_barrier(jnp.mean(value_rows * value_rows, axis=-1, keepdims=True)) + EPS) * gain

def rotary_tables(position, width):
    freq = jnp.exp(-jnp.log(jnp.float32(THETA)) * jnp.arange(0, width // 2).astype(jnp.float32) * 2.0 / width)
    angle = position.astype(jnp.float32)[:, None] * freq[None, :]
    angle = jnp.concatenate([angle, angle], axis=-1)
    return (jnp.cos(angle)[:, None, :], jnp.sin(angle)[:, None, :])

def rotate_halves(value_rows, cosine_table, sine_table):
    half = value_rows.shape[-1] // 2
    turned = jnp.concatenate([-value_rows[..., half:], value_rows[..., :half]], axis=-1)
    return value_rows * cosine_table + turned * sine_table

def attend_block(query_rows, keys, value_rows, mask):
    scale = 1.0 / jnp.sqrt(jnp.float32(HEAD_WIDTH))
    scores = jnp.einsum('qgrd,kgd->grqk', query_rows, keys, precision=lax.Precision.HIGHEST) * scale
    scores = lower_precision_back(scores)
    scores = jnp.where(mask[None, None], scores, NEG)
    probs = lower_precision(jax.nn.softmax(scores, axis=-1))
    return jnp.einsum('grqk,kgd->qgrd', probs, value_rows, precision=lax.Precision.HIGHEST)

def layer(resid, segment, position, params):
    gain_attn, w_query, key_weight, value_weight, w_headgate, query_norm_gain, gain_key, w_out, gain_mlp, w_gate, w_up, w_down = params
    total_count = resid.shape[0]
    repeat_heads = QUERY_HEADS // KEY_VALUE_HEADS
    normed_rows = lower_precision(root_mean_rows(resid, gain_attn))
    query_before_norm = lower_precision_back(matrix_product(normed_rows, w_query)).reshape(total_count, QUERY_HEADS, HEAD_WIDTH)
    key_before_norm = lower_precision_back(matrix_product(normed_rows, key_weight)).reshape(total_count, KEY_VALUE_HEADS, HEAD_WIDTH)
    value_rows = lower_precision(lower_precision_back(matrix_product(normed_rows, value_weight))).reshape(total_count, KEY_VALUE_HEADS, HEAD_WIDTH)
    gate_logit = lower_precision_back(matrix_product(normed_rows, w_headgate))
    cosine_table, sine_table = rotary_tables(position, HEAD_WIDTH)
    query_rows = lower_precision(rotate_halves(root_mean_rows(query_before_norm, query_norm_gain), cosine_table, sine_table)).reshape(total_count, KEY_VALUE_HEADS, repeat_heads, HEAD_WIDTH)
    keys = lower_precision(rotate_halves(root_mean_rows(key_before_norm, gain_key), cosine_table, sine_table))
    block = total_count // 2
    pieces = []
    for index in range(2):
        start = index * block
        reach = start + block
        row_ids = start + jnp.arange(block)
        key_ids = jnp.arange(reach)
        seg_rows = segment[start:reach]
        seg_keys = segment[:reach]
        mask = (key_ids[None, :] <= row_ids[:, None]) & ((seg_keys[None, :] == 0) | (seg_keys[None, :] == seg_rows[:, None]))
        pieces.append(jax.checkpoint(attend_block)(query_rows[start:reach], keys[:reach], value_rows[:reach], mask))
    attended = lower_precision_back(jnp.concatenate(pieces, axis=0).reshape(total_count, QUERY_HEADS, HEAD_WIDTH))
    gated = lower_precision(attended * jax.nn.sigmoid(gate_logit)[:, :, None]).reshape(total_count, QUERY_HEADS * HEAD_WIDTH)
    mid = resid + lower_precision_back(matrix_product(gated, w_out))
    mlp_normed = lower_precision(root_mean_rows(mid, gain_mlp))
    gate_pre = lower_precision_back(matrix_product(mlp_normed, w_gate))
    up_pre = lower_precision_back(matrix_product(mlp_normed, w_up))
    hidden = lower_precision(jax.nn.silu(gate_pre) * up_pre)
    return mid + matrix_product(hidden, w_down)

def reference(hidden_in, segment, position, attn_gain, w_query, key_weight, value_weight, w_headgate, query_gain, key_gain, w_out, mlp_gain, w_gate, w_up, w_down, cotangent):
    params = tuple((w.astype(jnp.float32) for w in (attn_gain, w_query, key_weight, value_weight, w_headgate, query_gain, key_gain, w_out, mlp_gain, w_gate, w_up, w_down)))
    groups = TOKENS // GROUP_TOK
    resid_all = hidden_in.astype(jnp.float32).reshape(groups, GROUP_TOK, MODEL_WIDTH)
    cot_all = cotangent.astype(jnp.float32).reshape(groups, GROUP_TOK, MODEL_WIDTH)
    seg_all = segment.reshape(groups, GROUP_TOK)
    pos_all = position.reshape(groups, GROUP_TOK)

    def one_group(carry, inputs):
        resid, seg_group, pos_group, cot_group = inputs
        result, pullback = jax.vjp(lambda xval, pval: layer(xval, seg_group, pos_group, pval), resid, params)
        grad_resid, grad_params = pullback(cot_group)
        carry = jax.tree.map(lambda left, right: left + right, carry, grad_params)
        return (carry, (result.astype(jnp.bfloat16), grad_resid.astype(jnp.bfloat16)))
    zeros = tuple((jnp.zeros(p.shape, jnp.float32) for p in params))
    totals, (outputs, input_grads) = lax.scan(one_group, zeros, (resid_all, seg_all, pos_all, cot_all))
    return (outputs.reshape(TOKENS, MODEL_WIDTH), input_grads.reshape(TOKENS, MODEL_WIDTH), totals[0], totals[1], totals[2], totals[3], totals[4], totals[5], totals[6], totals[7], totals[8], totals[9], totals[10], totals[11])
```

```python
import math

import jax
import jax.numpy as jnp
from jax import lax
from jax.sharding import PartitionSpec as P

EPS = 1e-06
THETA = 1000000.0
NEG = -1e30


def matrix_product(left, right):
    return jnp.dot(left, right, preferred_element_type=jnp.float32)


def lead_contract(left, right):
    return lax.dot_general(
        left, right, (((0,), (0,)), ((), ())), preferred_element_type=jnp.float32
    )


def tail_contract(left, right):
    return lax.dot_general(
        left, right, (((1,), (1,)), ((), ())), preferred_element_type=jnp.float32
    )


def root_mean_rows(value_rows, gain):
    return (
        value_rows
        * lax.rsqrt(jnp.mean(value_rows * value_rows, axis=-1, keepdims=True) + EPS)
        * gain
    )


def rotary_tables(position, width):
    freq = jnp.exp(
        -jnp.log(jnp.float32(THETA)) * jnp.arange(0, width // 2).astype(jnp.float32) * 2.0 / width
    )
    angle = position.astype(jnp.float32)[:, None] * freq[None, :]
    angle = jnp.concatenate([angle, angle], axis=-1)
    return (jnp.cos(angle)[:, None, :], jnp.sin(angle)[:, None, :])


def rotate_halves(value_rows, cosine_table, sine_table):
    half = value_rows.shape[-1] // 2
    turned = jnp.concatenate([-value_rows[..., half:], value_rows[..., :half]], axis=-1)
    return value_rows * cosine_table + turned * sine_table


def visible(segment, start, rows, reach):
    row_ids = start + jnp.arange(rows)
    key_ids = jnp.arange(reach)
    seg_rows = segment[start : start + rows]
    seg_keys = segment[:reach]
    return (key_ids[None, :] <= row_ids[:, None]) & (
        (seg_keys[None, :] == 0) | (seg_keys[None, :] == seg_rows[:, None])
    )


class Blocks:
    def __init__(self, size):
        self.size = size
        self.planes = size // 2
        self.index = lax.axis_index("dp")
        self.plane = self.index // 2
        self.side = self.index % 2

    def shift_pairs(self, shift):
        planes = self.planes
        return [
            (((plane + shift) % planes) * 2 + side, plane * 2 + side)
            for plane in range(planes)
            for side in range(2)
        ]

    def pull(self, value, shift):
        return lax.ppermute(value, "dp", self.shift_pairs(shift))

    def push(self, value, shift):
        return lax.ppermute(value, "dp", [(b, a) for a, b in self.shift_pairs(shift)])

    def swap(self, value):
        return lax.ppermute(value, "dp", [(i, i ^ 1) for i in range(self.size)])

    def gather(self, value):
        column = [value] + [self.pull(value, shift) for shift in range(1, self.planes)]
        return column + [self.swap(part) for part in column]

    def absolute(self, place):
        near, shift = divmod(place, self.planes)
        side = (self.side + near) % 2
        return lax.rem(self.plane + shift, self.planes) * 2 + side

    def relative(self, block):
        plane, side = divmod(block, 2)
        near = (side + self.side) % 2
        return near * self.planes + lax.rem(plane + self.planes - self.plane, self.planes)

    def take(self, value, places):
        width = value.shape[-1] // self.size
        return jnp.concatenate(
            [
                lax.dynamic_slice_in_dim(value, place * width, width, axis=value.ndim - 1)
                for place in places
            ],
            axis=-1,
        )

    def to_relative(self, value):
        return self.take(value, [self.absolute(place) for place in range(self.size)])

    def to_absolute(self, value):
        return self.take(value, [self.relative(block) for block in range(self.size)])

    def scatter(self, far, near):
        f32 = jnp.float32
        got = [self.swap(part) for part in far]
        total = near[0] + got[0].astype(f32)
        for shift in range(1, self.planes):
            joined = (near[shift] + got[shift].astype(f32)).astype(jnp.bfloat16)
            total = total + self.push(joined, shift).astype(f32)
        return total

    def total(self, value):
        value = value + self.swap(value)
        step = 1
        while step < self.planes:
            pairs = [
                (plane * 2 + side, (plane ^ step) * 2 + side)
                for plane in range(self.planes)
                for side in range(2)
            ]
            value = value + lax.ppermute(value, "dp", pairs)
            step *= 2
        return value


def cut(value, count, axis):
    return jnp.split(value, count, axis=axis)


def local(
    hidden_in,
    segment,
    position,
    attn_gain,
    w_query,
    key_weight,
    value_weight,
    w_headgate,
    query_gain,
    key_gain,
    w_out,
    mlp_gain,
    w_gate,
    w_up,
    w_down,
    cotangent,
):
    bf16 = jnp.bfloat16
    f32 = jnp.float32
    dp = lax.axis_size("dp")
    tp = lax.axis_size("tensor")
    blocks = Blocks(dp)
    planes = blocks.planes
    own = w_query.shape[0]
    model = own * dp
    half = model // 2
    head_own = query_gain.shape[0]
    head_size = head_own * dp
    heads_query = w_headgate.shape[1]
    width_query = w_query.shape[1]
    width_kv = key_weight.shape[1]
    heads_kv = width_kv // head_size
    repeat_heads = heads_query // heads_kv
    scale = 1.0 / math.sqrt(head_size)

    small = jnp.concatenate(
        [
            attn_gain[None],
            mlp_gain[None],
            jnp.pad(jnp.concatenate([query_gain, key_gain])[None], ((0, 0), (0, own - 2 * head_own))),
            w_headgate.T,
        ],
        axis=0,
    )
    small_parts = blocks.gather(small)
    qkv_parts = blocks.gather(jnp.concatenate([w_query, key_weight, value_weight], axis=1))
    out_parts = blocks.gather(w_out)
    down_parts = blocks.gather(w_down)
    gate_parts = blocks.gather(w_gate)
    up_parts = blocks.gather(w_up)

    small_full = jnp.concatenate(small_parts, axis=1)
    attn_scale = small_full[0].astype(f32)
    mlp_scale = small_full[1].astype(f32)
    full_headgate = small_full[3:]
    head_gains = jnp.stack([part[2, : 2 * head_own] for part in small_parts])
    head_gains = jnp.concatenate(
        [
            lax.dynamic_slice_in_dim(head_gains, blocks.relative(block), 1, axis=0)
            for block in range(dp)
        ],
        axis=0,
    )
    query_scale = head_gains[:, :head_own].reshape(head_size).astype(f32)
    key_scale = head_gains[:, head_own:].reshape(head_size).astype(f32)

    resid = blocks.to_relative(hidden_in).astype(f32)
    cot = blocks.to_relative(cotangent)
    normed_rows = lax.all_gather(
        root_mean_rows(resid, attn_scale).astype(bf16), "tensor", axis=0, tiled=True
    )
    out_grad = lax.all_gather(cot, "tensor", axis=0, tiled=True)
    total_count = normed_rows.shape[0]
    cosine_table, sine_table = rotary_tables(position, head_size)

    def query_prep(projected, gain):
        return rotate_halves(root_mean_rows(projected, gain), cosine_table, sine_table)

    full_qkv = jnp.concatenate(qkv_parts, axis=0)
    projected = matrix_product(normed_rows, full_qkv)
    query_before_norm = projected[:, :width_query].reshape(total_count, heads_query, head_size)
    key_before_norm = projected[:, width_query : width_query + width_kv].reshape(
        total_count, heads_kv, head_size
    )
    value_rows = (
        projected[:, width_query + width_kv :]
        .astype(bf16)
        .reshape(total_count, heads_kv, head_size)
    )
    gate_logit = tail_contract(normed_rows, full_headgate)
    query_rows = (
        query_prep(query_before_norm, query_scale)
        .astype(bf16)
        .reshape(total_count, heads_kv, repeat_heads, head_size)
    )
    keys_rot = query_prep(key_before_norm, key_scale).astype(bf16)
    block = total_count // 2
    outputs = []
    log_sums = []
    for index in range(2):
        start = index * block
        reach = start + block
        mask = visible(segment, start, block, reach)
        scores = (
            jnp.einsum(
                "qgrd,kgd->grqk",
                query_rows[start:reach],
                keys_rot[:reach],
                preferred_element_type=f32,
            )
            * scale
        )
        scores = jnp.where(mask[None, None], scores, NEG)
        top = jnp.max(scores, axis=-1, keepdims=True)
        expd = jnp.exp(scores - top)
        denom = jnp.sum(expd, axis=-1, keepdims=True)
        weights = (expd / denom).astype(bf16)
        outputs.append(
            jnp.einsum("grqk,kgd->qgrd", weights, value_rows[:reach], preferred_element_type=f32)
        )
        log_sums.append(top + jnp.log(denom))
    attended = jnp.concatenate(outputs, axis=0).reshape(total_count, heads_query, head_size)
    gate_prob = jax.nn.sigmoid(gate_logit)
    gated = (
        (attended * gate_prob[:, :, None])
        .astype(bf16)
        .reshape(total_count, heads_query * head_size)
    )
    full_out = jnp.concatenate(out_parts, axis=1)
    attn_part = lax.psum_scatter(
        matrix_product(gated, full_out).astype(bf16), "tensor", scatter_dimension=0, tiled=True
    ).astype(f32)
    mid = resid + attn_part
    mlp_normed = lax.all_gather(
        root_mean_rows(mid, mlp_scale).astype(bf16), "tensor", axis=0, tiled=True
    )
    full_gate = jnp.concatenate(gate_parts, axis=0)
    full_up = jnp.concatenate(up_parts, axis=0)
    full_down = jnp.concatenate(down_parts, axis=1)
    gate_pre = matrix_product(mlp_normed, full_gate)
    up_pre = matrix_product(mlp_normed, full_up)
    hidden = (jax.nn.silu(gate_pre) * up_pre).astype(bf16)
    mlp_part = lax.psum_scatter(
        matrix_product(hidden, full_down).astype(bf16), "tensor", scatter_dimension=0, tiled=True
    ).astype(f32)
    layer_out = blocks.to_absolute((mid + mlp_part).astype(bf16))

    def weight_grad_rows(left, right):
        far = lead_contract(left[:, half:], right).astype(bf16)
        near = lead_contract(left[:, :half], right)
        return blocks.scatter(cut(far, planes, 0), cut(near, planes, 0))

    def weight_grad_columns(left, right):
        far = lead_contract(left, right[:, half:]).astype(bf16)
        near = lead_contract(left, right[:, :half])
        return blocks.scatter(cut(far, planes, 1), cut(near, planes, 1))

    grad_down = weight_grad_columns(hidden, out_grad)
    grad_hidden = tail_contract(out_grad, full_down)
    sigma = jax.nn.sigmoid(gate_pre)
    grad_gate_pre = (grad_hidden * up_pre * sigma * (1.0 + gate_pre * (1.0 - sigma))).astype(bf16)
    grad_up_pre = (grad_hidden * gate_pre * sigma).astype(bf16)
    mlp_norm_part = tail_contract(grad_gate_pre, full_gate) + tail_contract(grad_up_pre, full_up)
    mlp_norm_grad = lax.psum_scatter(
        mlp_norm_part.astype(bf16), "tensor", scatter_dimension=0, tiled=True
    ).astype(f32)
    grad_gate = weight_grad_rows(mlp_normed, grad_gate_pre)
    grad_up = weight_grad_rows(mlp_normed, grad_up_pre)
    unused_mid, mlp_pull = jax.vjp(root_mean_rows, mid, mlp_scale)
    mid_norm_grad, mlp_gain_term = mlp_pull(mlp_norm_grad)
    mid_grad = cot.astype(f32) + mid_norm_grad
    branch_grad = lax.all_gather(mid_grad.astype(bf16), "tensor", axis=0, tiled=True)
    grad_out = weight_grad_columns(gated, branch_grad)
    gated_grad = tail_contract(branch_grad, full_out).reshape(total_count, heads_query, head_size)
    attended_grad = (
        (gated_grad * gate_prob[:, :, None])
        .astype(bf16)
        .reshape(total_count, heads_kv, repeat_heads, head_size)
    )
    logit_grad = (jnp.sum(gated_grad * attended, axis=-1) * gate_prob * (1.0 - gate_prob)).astype(
        bf16
    )
    query_parts = []
    key_grad = jnp.zeros((total_count, heads_kv, head_size), f32)
    value_grad = jnp.zeros((total_count, heads_kv, head_size), f32)
    for index in range(2):
        start = index * block
        reach = start + block
        mask = visible(segment, start, block, reach)
        scores = (
            jnp.einsum(
                "qgrd,kgd->grqk",
                query_rows[start:reach],
                keys_rot[:reach],
                preferred_element_type=f32,
            )
            * scale
        )
        scores = jnp.where(mask[None, None], scores, NEG)
        probs = jnp.exp(scores - log_sums[index])
        prob_grad = jnp.einsum(
            "qgrd,kgd->grqk",
            attended_grad[start:reach],
            value_rows[:reach],
            preferred_element_type=f32,
        )
        delta = jnp.sum(probs * prob_grad, axis=-1, keepdims=True)
        score_grad = (probs * (prob_grad - delta)).astype(bf16)
        query_parts.append(
            jnp.einsum("grqk,kgd->qgrd", score_grad, keys_rot[:reach], preferred_element_type=f32)
            * scale
        )
        key_grad = key_grad.at[:reach].add(
            jnp.einsum(
                "grqk,qgrd->kgd", score_grad, query_rows[start:reach], preferred_element_type=f32
            )
            * scale
        )
        value_grad = value_grad.at[:reach].add(
            jnp.einsum(
                "grqk,qgrd->kgd",
                probs.astype(bf16),
                attended_grad[start:reach],
                preferred_element_type=f32,
            )
        )
    query_rot_grad = jnp.concatenate(query_parts, axis=0).reshape(
        total_count, heads_query, head_size
    )
    unused_query, query_pull = jax.vjp(query_prep, query_before_norm, query_scale)
    query_pre_grad, query_gain_term = query_pull(query_rot_grad)
    unused_key, key_pull = jax.vjp(query_prep, key_before_norm, key_scale)
    key_pre_grad, key_gain_term = key_pull(key_grad)
    pre_low = jnp.concatenate(
        [
            query_pre_grad.astype(bf16).reshape(total_count, width_query),
            key_pre_grad.astype(bf16).reshape(total_count, width_kv),
            value_grad.astype(bf16).reshape(total_count, width_kv),
        ],
        axis=1,
    )
    norm_part = tail_contract(pre_low, full_qkv) + matrix_product(logit_grad, full_headgate)
    norm_grad = lax.psum_scatter(
        norm_part.astype(bf16), "tensor", scatter_dimension=0, tiled=True
    ).astype(f32)
    grad_qkv = weight_grad_rows(normed_rows, pre_low)
    headgate_term = lead_contract(logit_grad, normed_rows)
    unused_resid, attn_pull = jax.vjp(root_mean_rows, resid, attn_scale)
    resid_norm_grad, attn_gain_term = attn_pull(norm_grad)
    grad_in = blocks.to_absolute((mid_grad + resid_norm_grad).astype(bf16))

    head_terms = jnp.concatenate([query_gain_term, key_gain_term])
    terms = jnp.concatenate(
        [
            blocks.to_absolute(
                jnp.concatenate([attn_gain_term[None], mlp_gain_term[None], headgate_term], axis=0)
            ),
            jnp.pad(head_terms, (0, model - 2 * head_size))[None],
        ],
        axis=0,
    )
    terms = blocks.total(terms)
    gain_terms = jnp.concatenate([terms[:2], terms[2 + heads_query :]], axis=0)
    step = 1
    while step < tp:
        gain_terms = gain_terms + lax.ppermute(
            gain_terms, "tensor", [(i, i ^ step) for i in range(tp)]
        )
        step *= 2
    mine = lax.dynamic_slice_in_dim(terms, blocks.index * own, own, axis=1)
    gain_mine = lax.dynamic_slice_in_dim(gain_terms, blocks.index * own, own, axis=1)
    grad_headgate = mine[2 : 2 + heads_query].T
    grad_query_gain = lax.dynamic_slice_in_dim(
        gain_terms[2, :head_size], blocks.index * head_own, head_own, axis=0
    )
    grad_key_gain = lax.dynamic_slice_in_dim(
        gain_terms[2, head_size : 2 * head_size], blocks.index * head_own, head_own, axis=0
    )
    return (
        layer_out,
        grad_in,
        gain_mine[0],
        grad_qkv[:, :width_query],
        grad_qkv[:, width_query : width_query + width_kv],
        grad_qkv[:, width_query + width_kv :],
        grad_headgate,
        grad_query_gain,
        grad_key_gain,
        grad_out,
        gain_mine[1],
        grad_gate,
        grad_up,
        grad_down,
    )


def solution(mesh):
    placed = (
        P(("dp", "tensor"), None),
        P("dp"),
        P("dp"),
        P("dp"),
        P("dp", "tensor"),
        P("dp", "tensor"),
        P("dp", "tensor"),
        P("dp", "tensor"),
        P("dp"),
        P("dp"),
        P("tensor", "dp"),
        P("dp"),
        P("dp", "tensor"),
        P("dp", "tensor"),
        P("tensor", "dp"),
        P(("dp", "tensor"), None),
    )
    return jax.shard_map(
        local,
        mesh=mesh,
        in_specs=placed,
        out_specs=(
            P(("dp", "tensor"), None),
            P(("dp", "tensor"), None),
            P("dp"),
            P("dp", "tensor"),
            P("dp", "tensor"),
            P("dp", "tensor"),
            P("dp", "tensor"),
            P("dp"),
            P("dp"),
            P("tensor", "dp"),
            P("dp"),
            P("dp", "tensor"),
            P("dp", "tensor"),
            P("tensor", "dp"),
        ),
        check_vma=False,
    )
```
